32 devices in a mesh: gx: 2 (over x), gy: 4 (over z), gz: 4 (over y, core).
Axes of the slice: x: 2, y: 2, z: 4, core: 2. Of those that a mesh axis runs over, the one named last changes fastest.
Arguments:
- vectors: float32 [3, 12, 24, 24, 128], P(None, 'gx', 'gy', 'gz'), may hold values from -6 to 6
- orient_flip: int32 [4, 8, 1152], P('gx', 'gy', 'gz'), may hold values from 0 to 1
- reluctivity: float32 [4, 8, 512], P('gx', 'gy', 'gz'), may hold values from 0.05 to 0.5
- conductivity: float32 [4, 8, 512], P('gx', 'gy', 'gz'), may hold values from 1 to 10
Outputs:
- out_x: float32 [12, 28, 28, 128], P('gx', 'gy', 'gz')
- out_y: float32 [14, 24, 28, 128], P('gx', 'gy', 'gz')
- out_z: float32 [14, 28, 24, 128], P('gx', 'gy', 'gz')
The draws below stay inside these ranges and needn't reach their ends.
Inputs may be any that keep to these rules, and one draw needn't show every extreme that they name: `orient_flip`: 1 reverses the orientation of that degree of freedom in that element, 0 keeps it.
All inputs are finite; a program needn't handle non-finite values.
Results may differ from the reference program's by a relative error of at most 0.00007.
Values sent between devices are 32-bit elements; how exact they have to be, the bound alone decides.
A program may use at most 64 MiB of HBM per device.

```python
import math
import jax
import jax.numpy as jnp
import numpy as np
from jax import lax

ORDER = 3
QUAD = 4
VECS = 128
NX = 4
NY = 8
NZ = 8
ELEM_DOFS = 144
QPTS = 64
N_GX = 2
N_GY = 4
N_GZ = 4


def touch_ends(entries, key, low, high):
    place = [jax.random.randint(jax.random.fold_in(key, axis), (), 0, length) for axis, length in enumerate(entries.shape)]
    widest = entries.shape.index(max(entries.shape))
    neighbour = place[:widest] + [(place[widest] + 1) % entries.shape[widest]] + place[widest + 1:]
    return entries.at[tuple(place)].set(low).at[tuple(neighbour)].set(high)


def levels(key, shape, shards, least, largest):
    gain, own = 1.0, jax.random.fold_in(key, 6)
    for axis_at, parts in shards:
        heights = jnp.exp(jax.random.uniform(jax.random.fold_in(own, axis_at), (parts,), jnp.float32, least / len(shards), largest / len(shards)))
        gain = gain * jnp.repeat(heights, shape[axis_at] // parts).reshape([-1 if axis == axis_at else 1 for axis in range(len(shape))])
    return gain


def scatter_about(own_key, shape, scale, most, pieces=(), kind=jnp.bfloat16):
    entries = jax.random.normal(own_key, shape, jnp.float32) * scale
    if len(pieces) > 0:
        entries = levels(own_key, shape, pieces, -0.22, 0.18) * entries
    return jnp.clip(entries, min=-most, max=most).astype(kind)


def setup_inputs(seed: int = 0) -> dict:
    key_of = jax.random.split(jax.random.key(seed), 5)
    vectors = scatter_about(key_of[0], (3, NX * ORDER, NY * ORDER, NZ * ORDER, VECS), 1.0, 6.0, ((1, 2), (2, 4), (3, 4)), jnp.float32)
    orient_flip = touch_ends(jax.random.randint(key_of[1], (NX, NY, NZ * ELEM_DOFS), 0, 2), jax.random.fold_in(key_of[1], 1), 0, 1).astype(jnp.int32)
    reluctivity = jnp.clip(jnp.exp(math.log(0.5) - 2.3025851 * jax.random.uniform(key_of[2], (NX, NY, NZ * QPTS), jnp.float32) ** levels(key_of[2], (NX, NY, NZ * QPTS), ((0, 2), (1, 4), (2, 4)), -0.2, 0.2)), 0.05, 0.5)
    conductivity = jnp.clip(jnp.exp(math.log(10.0) - 2.3025851 * jax.random.uniform(key_of[3], (NX, NY, NZ * QPTS), jnp.float32) ** levels(key_of[3], (NX, NY, NZ * QPTS), ((0, 2), (1, 4), (2, 4)), -0.2, 0.2)), 1.0, 10.0)
    return {"vectors": vectors, "orient_flip": orient_flip, "reluctivity": reluctivity, "conductivity": conductivity}


def lagrange(points_at, evaluate_at):
    amount = len(points_at)
    values = np.ones((len(evaluate_at), amount))
    slopes = np.zeros((len(evaluate_at), amount))
    for which in range(amount):
        for column in range(amount):
            if column != which:
                factor = (evaluate_at - points_at[column]) / (points_at[which] - points_at[column])
                slopes[:, which] = slopes[:, which] * factor + values[:, which] / (points_at[which] - points_at[column])
                values[:, which] = values[:, which] * factor
    return (values, slopes)

def basis_tables():
    lobatto = np.array([0.0, (1 - 5 ** (-0.5)) / 2, (1 + 5 ** (-0.5)) / 2, 1.0])
    gauss_open = np.array([(1 - 0.6 ** 0.5) / 2, 0.5, (1 + 0.6 ** 0.5) / 2])
    inner_pt = (3.0 / 7 - 2.0 / 7 * (6.0 / 5) ** 0.5) ** 0.5
    outer_pt = (3.0 / 7 + 2.0 / 7 * (6.0 / 5) ** 0.5) ** 0.5
    inner_wt = (18 + 30 ** 0.5) / 36
    outer_wt = (18 - 30 ** 0.5) / 36
    quad_points = (1 + np.array([-outer_pt, -inner_pt, inner_pt, outer_pt])) / 2
    quad_weight = np.array([outer_wt, inner_wt, inner_wt, outer_wt]) / 2
    closed, slopes = lagrange(lobatto, quad_points)
    opened, unused_slopes = lagrange(gauss_open, quad_points)
    weight_cube = quad_weight[:, None, None, None, None] * quad_weight[None, :, None, None, None] * quad_weight[None, None, :, None, None]
    return (jnp.asarray(closed, dtype=jnp.float32), jnp.asarray(slopes, dtype=jnp.float32), jnp.asarray(opened, dtype=jnp.float32), jnp.asarray(weight_cube, dtype=jnp.float32))

def contract(tensor, first_mat, second_mat, third_mat):
    section_one = jnp.einsum('qa,abcef->qbcef', first_mat, tensor, precision=lax.Precision.HIGHEST)
    section_two = jnp.einsum('rb,qbcef->qrcef', second_mat, section_one, precision=lax.Precision.HIGHEST)
    return jnp.einsum('sc,qrcef->qrsef', third_mat, section_two, precision=lax.Precision.HIGHEST)

def evaluate(elem_x, elem_y, elem_z, closed, slopes, opened):
    u_x = contract(elem_x, opened, closed, closed)
    u_y = contract(elem_y, closed, opened, closed)
    u_z = contract(elem_z, closed, closed, opened)
    deriv_xy = contract(elem_x, opened, slopes, closed)
    deriv_xz = contract(elem_x, opened, closed, slopes)
    deriv_yx = contract(elem_y, slopes, opened, closed)
    deriv_yz = contract(elem_y, closed, opened, slopes)
    deriv_zx = contract(elem_z, slopes, closed, opened)
    deriv_zy = contract(elem_z, closed, slopes, opened)
    return (u_x, u_y, u_z, deriv_zy - deriv_yz, deriv_xz - deriv_zx, deriv_yx - deriv_xy)

def windows(array, axis, amount, open_dim):
    dims_now = array.shape
    if open_dim:
        split = array.reshape(dims_now[:axis] + (amount, ORDER) + dims_now[axis + 1:])
        return jnp.swapaxes(split, axis, axis + 1)
    reach = ORDER * (amount - 1) + 1
    return jnp.stack([lax.slice_in_dim(array, offset, offset + reach, ORDER, axis) for offset in range(ORDER + 1)], axis=axis)

def collect(array, open_axis, counts):
    result = array
    for axis in range(3):
        result = windows(result, 2 * axis, counts[axis], axis == open_axis)
    dims_now = result.shape
    result = jnp.transpose(result, (0, 2, 4, 1, 3, 5, 6))
    return result.reshape(dims_now[0], dims_now[2], dims_now[4], counts[0] * counts[1] * counts[2], dims_now[6])

def element_data(orient_flip, reluctivity, conductivity, elements):
    flip_float = orient_flip.reshape(elements, ELEM_DOFS).T.astype(jnp.float32)
    sign_all = 1.0 - 2.0 * flip_float
    per_comp = ORDER * (ORDER + 1) * (ORDER + 1)
    sign_x = sign_all[:per_comp].reshape(ORDER, ORDER + 1, ORDER + 1, elements, 1)
    sign_y = sign_all[per_comp:2 * per_comp].reshape(ORDER + 1, ORDER, ORDER + 1, elements, 1)
    sign_z = sign_all[2 * per_comp:].reshape(ORDER + 1, ORDER + 1, ORDER, elements, 1)
    reluct = reluctivity.reshape(elements, QPTS).T.reshape(QUAD, QUAD, QUAD, elements, 1)
    conduct = conductivity.reshape(elements, QPTS).T.reshape(QUAD, QUAD, QUAD, elements, 1)
    return (sign_x, sign_y, sign_z, reluct, conduct)

def element_apply(lvec_x, lvec_y, lvec_z, data, counts):

    def gather_all(part_x, part_y, part_z):
        return (collect(part_x, 0, counts), collect(part_y, 1, counts), collect(part_z, 2, counts))
    elems, scatter_back = jax.vjp(gather_all, lvec_x, lvec_y, lvec_z)
    sign_x, sign_y, sign_z, reluct, conduct = data
    closed, slopes, opened, weight_cube = basis_tables()

    def forward(part_x, part_y, part_z):
        return evaluate(part_x, part_y, part_z, closed, slopes, opened)
    quads, pullback = jax.vjp(forward, elems[0] * sign_x, elems[1] * sign_y, elems[2] * sign_z)
    mass_scale = weight_cube * conduct
    curl_scale = weight_cube * reluct
    cotangent = (mass_scale * quads[0], mass_scale * quads[1], mass_scale * quads[2], curl_scale * quads[3], curl_scale * quads[4], curl_scale * quads[5])
    grads = pullback(cotangent)
    return scatter_back((grads[0] * sign_x, grads[1] * sign_y, grads[2] * sign_z))

def extend(array, axes):
    for axis in axes:
        array = jnp.concatenate([array, lax.slice_in_dim(array, 0, 1, 1, axis)], axis)
    return array

def fold_back(array, axes):
    for axis in axes:
        total_len = array.shape[axis]
        head_sum = lax.slice_in_dim(array, 0, 1, 1, axis) + lax.slice_in_dim(array, total_len - 1, total_len, 1, axis)
        array = jnp.concatenate([head_sum, lax.slice_in_dim(array, 1, total_len - 1, 1, axis)], axis)
    return array

def spread(array, axis, blocks):
    dims_now = array.shape
    block_len = dims_now[axis] // blocks
    split = array.reshape(dims_now[:axis] + (blocks, block_len) + dims_now[axis + 1:])
    following = jnp.roll(lax.slice_in_dim(split, 0, 1, 1, axis + 1), -1, axis)
    joined = jnp.concatenate([split, following], axis + 1)
    return joined.reshape(dims_now[:axis] + (blocks * (block_len + 1),) + dims_now[axis + 1:])

def reference(vectors, orient_flip, reluctivity, conductivity):
    data = element_data(orient_flip, reluctivity, conductivity, NX * NY * NZ)
    group = math.gcd(VECS, 2)
    dims_now = vectors.shape
    grouped = jnp.moveaxis(vectors.reshape(dims_now[:4] + (VECS // group, group)), 4, 0)

    def apply_whole(single):
        results = element_apply(extend(single[0], (1, 2)), extend(single[1], (0, 2)), extend(single[2], (0, 1)), data, (NX, NY, NZ))
        own_x = fold_back(results[0], (1, 2))
        own_y = fold_back(results[1], (0, 2))
        own_z = fold_back(results[2], (0, 1))
        return (spread(spread(own_x, 1, N_GY), 2, N_GZ), spread(spread(own_y, 0, N_GX), 2, N_GZ), spread(spread(own_z, 0, N_GX), 1, N_GY))
    parts_x, parts_y, parts_z = lax.map(apply_whole, grouped)

    def unite(stacked):
        moved = jnp.moveaxis(stacked, 0, 3)
        shape_now = moved.shape
        return moved.reshape(shape_now[:3] + (VECS,))
    return (unite(parts_x), unite(parts_y), unite(parts_z))
```

```python
import functools
import jax
import jax.numpy as jnp
import numpy as np
from jax import lax
from jax.experimental import pallas as pl
from jax.experimental.pallas import tpu as pltpu
from jax.sharding import PartitionSpec as P

ORDER = 3
QUAD = 4
ELEM_DOFS = 144
QPTS = 64
AXES = ("gx", "gy", "gz")
MESH = pl.DeviceIdType.MESH


def lagrange(points_at, evaluate_at):
    amount = len(points_at)
    values = np.ones((len(evaluate_at), amount))
    slopes = np.zeros((len(evaluate_at), amount))
    for which in range(amount):
        for column in range(amount):
            if column != which:
                factor = (evaluate_at - points_at[column]) / (points_at[which] - points_at[column])
                slopes[:, which] = slopes[:, which] * factor + values[:, which] / (
                    points_at[which] - points_at[column]
                )
                values[:, which] = values[:, which] * factor
    return (values, slopes)


def basis_tables():
    lobatto = np.array([0.0, (1 - 5 ** (-0.5)) / 2, (1 + 5 ** (-0.5)) / 2, 1.0])
    gauss_open = np.array([(1 - 0.6**0.5) / 2, 0.5, (1 + 0.6**0.5) / 2])
    inner_pt = (3.0 / 7 - 2.0 / 7 * (6.0 / 5) ** 0.5) ** 0.5
    outer_pt = (3.0 / 7 + 2.0 / 7 * (6.0 / 5) ** 0.5) ** 0.5
    inner_wt = (18 + 30**0.5) / 36
    outer_wt = (18 - 30**0.5) / 36
    quad_points = (1 + np.array([-outer_pt, -inner_pt, inner_pt, outer_pt])) / 2
    quad_weight = np.array([outer_wt, inner_wt, inner_wt, outer_wt]) / 2
    closed, _ = lagrange(lobatto, quad_points)
    opened, _ = lagrange(gauss_open, quad_points)
    _, colloc = lagrange(quad_points, quad_points)
    return closed, opened, colloc, quad_weight


CLOSED, OPENED, COLLOC, WEIGHT = basis_tables()


def add_all(terms):
    total = terms[0]
    for term in terms[1:]:
        total = total + term
    return total


def apply(mat, xs, sigma=1):
    rows, cols = mat.shape
    half = cols // 2
    plus = [xs[p] + xs[cols - 1 - p] for p in range(half)]
    minus = [xs[p] - xs[cols - 1 - p] for p in range(half)]
    ys = [None] * rows
    for q in range((rows + 1) // 2):
        even_c = [(mat[q, p] + mat[q, cols - 1 - p]) / 2 for p in range(half)]
        odd_c = [(mat[q, p] - mat[q, cols - 1 - p]) / 2 for p in range(half)]
        even = [np.float32(c) * s for c, s in zip(even_c, plus)]
        if cols % 2:
            even.append(np.float32(mat[q, half]) * xs[half])
        even = add_all(even)
        if 2 * q == rows - 1:
            ys[q] = even
            continue
        odd = add_all([np.float32(c) * d for c, d in zip(odd_c, minus)])
        ys[q] = even + odd
        ys[rows - 1 - q] = even - odd if sigma > 0 else odd - even
    return ys


def swap(blocks, size):
    count = blocks[0].shape[0] // size
    return [
        jnp.concatenate([b[q * size : (q + 1) * size] for b in blocks], 0) for q in range(count)
    ]


def dims_of(comp):
    return [ORDER if axis == comp else ORDER + 1 for axis in range(3)]


def kernel(
    mesh_sizes, vec, flip, reluct, conduct, out_x, out_y, out_z,
    elem, sign, mass, curlw, flat, tmp, uq, cq,
    res_x, res_y, res_z, pack1, corner1, hx, hy, hz, hc, pack2_x, pack2_y, corner2,
    rim_xy, rim_xz, rim_yx, rim_yz, rim_zx, rim_zy, rc,
    s1, r1, s2, r2,
):
    f32 = jnp.float32
    cx, cy = flip.shape[0], flip.shape[1]
    cz = flip.shape[2] // ELEM_DOFS
    counts = (cx, cy, cz)
    ne = cx * cy * cz
    size = tuple(ORDER * c for c in counts)
    me = [lax.axis_index(a) for a in AXES]

    def device(shift):
        return tuple(
            lax.rem(me[a] + (shift[a] + mesh_sizes[a]), mesh_sizes[a]) for a in range(3)
        )

    offsets = []
    for dx in (-1, 0, 1):
        for dy in (-1, 0, 1):
            for dz in (-1, 0, 1):
                if 1 <= abs(dx) + abs(dy) + abs(dz) <= 2:
                    offsets.append((dx, dy, dz))
    barrier = pltpu.get_barrier_semaphore()
    for shift in offsets:
        pl.semaphore_signal(barrier, inc=1, device_id=device(shift), device_id_type=MESH)

    for comp in (0, 1):
        for x in range(size[0]):
            for y in range(size[1]):
                pack1[comp, x, y : y + 1, :] = vec[comp, x, y, 0:1, :]
    for x in range(size[0]):
        corner1[0, x : x + 1, :] = vec[0, x, 0, 0:1, :]
    for y in range(size[1]):
        corner1[1, y : y + 1, :] = vec[1, 0, y, 0:1, :]
    pl.semaphore_wait(barrier, len(offsets))

    copies = []

    def send(src, dst, shift, sends, recvs, which):
        copy = pltpu.make_async_remote_copy(
            src_ref=src, dst_ref=dst, send_sem=sends.at[which], recv_sem=recvs.at[which],
            device_id=device(shift), device_id_type=MESH,
        )
        copy.start()
        return copy

    one = [
        send(vec.at[0, :, 0], hy.at[0], (0, -1, 0), s1, r1, 0),
        send(vec.at[2, :, 0], hy.at[1], (0, -1, 0), s1, r1, 1),
        send(vec.at[1:3, 0], hx, (-1, 0, 0), s1, r1, 2),
        send(pack1, hz, (0, 0, -1), s1, r1, 3),
        send(corner1.at[0], hc.at[0], (0, -1, -1), s1, r1, 4),
        send(corner1.at[1], hc.at[1], (-1, 0, -1), s1, r1, 5),
        send(vec.at[2, 0, 0], hc.at[2], (-1, -1, 0), s1, r1, 6),
    ]

    for i in range(cx):
        for j in range(cy):
            for k in range(cz):
                e = (i * cy + j) * cz + k
                flat[0, e : e + 1, 0:ELEM_DOFS] = 1.0 - 2.0 * flip[
                    i, j : j + 1, k * ELEM_DOFS : (k + 1) * ELEM_DOFS
                ].astype(f32)
                flat[1, e : e + 1, 0:QPTS] = reluct[i, j : j + 1, k * QPTS : (k + 1) * QPTS]
                flat[2, e : e + 1, 0:QPTS] = conduct[i, j : j + 1, k * QPTS : (k + 1) * QPTS]
    lanes = vec.shape[-1]
    for d in range(ELEM_DOFS):
        sign[d * ne : (d + 1) * ne, :] = jnp.broadcast_to(flat[0, :, d : d + 1], (ne, lanes))
    for q in range(QPTS):
        w = np.float32(WEIGHT[q // 16] * WEIGHT[q // 4 % 4] * WEIGHT[q % 4])
        rows = slice(q * ne, (q + 1) * ne)
        curlw[rows, :] = jnp.broadcast_to(flat[1, :, q : q + 1] * w, (ne, lanes))
        mass[rows, :] = jnp.broadcast_to(flat[2, :, q : q + 1] * w, (ne, lanes))

    def homes(comp, axis, low, high):
        found = []
        for el in range(counts[axis]):
            first = max(low, ORDER * el)
            last = min(high, ORDER * el + dims_of(comp)[axis])
            if first < last:
                found.append((el, first - ORDER * el, first - low, last - first))
        return found

    def places(comp, axis, at, low, high):
        dims = dims_of(comp)
        steps = (dims[1] * dims[2], dims[2], 1)
        span = [(p, p + 1) for p in at]
        span[axis] = (low, high)
        for fx in homes(comp, 0, *span[0]):
            for fy in homes(comp, 1, *span[1]):
                for fz in homes(comp, 2, *span[2]):
                    found = (fx, fy, fz)
                    e = (fx[0] * cy + fy[0]) * cz + fz[0]
                    d = comp * 48 + sum(found[t][1] * steps[t] for t in range(3))
                    yield found[axis][2], found[axis][3], d * ne + e, steps[axis] * ne

    def put(comp, axis, at, low, high, load):
        for offset, length, row, stride in places(comp, axis, at, low, high):
            elem[pl.ds(row, length, stride=stride), :] = load(offset, offset + length)

    for comp in range(3):
        for x in range(size[0]):
            for y in range(size[1]):
                put(comp, 2, (x, y, 0), 0, size[2], lambda a, b: vec[comp, x, y, a:b, :])

    for copy in one:
        copy.wait_recv()
    for slot, comp in ((0, 0), (1, 2)):
        for x in range(size[0]):
            put(comp, 2, (x, size[1], 0), 0, size[2], lambda a, b: hy[slot, x, a:b, :])
    for slot, comp in ((0, 1), (1, 2)):
        for y in range(size[1]):
            put(comp, 2, (size[0], y, 0), 0, size[2], lambda a, b: hx[slot, y, a:b, :])
    for comp in (0, 1):
        for x in range(size[0]):
            put(comp, 1, (x, 0, size[2]), 0, size[1], lambda a, b: hz[comp, x, a:b, :])
    put(0, 0, (0, size[1], size[2]), 0, size[0], lambda a, b: hc[0, a:b, :])
    put(1, 1, (size[0], 0, size[2]), 0, size[1], lambda a, b: hc[1, a:b, :])
    put(2, 2, (size[0], size[1], 0), 0, size[2], lambda a, b: hc[2, a:b, :])

    def rows_of(axis, at, line, dims):
        others = [t for t in range(3) if t != axis]
        points = []
        for last in range(dims[others[1]]):
            index = [0, 0, 0]
            index[axis], index[others[0]], index[others[1]] = at, line, last
            points.append(((index[0] * dims[1] + index[1]) * dims[2] + index[2]) * ne)
        return points

    def load_line(ref, base, axis, at, line, dims):
        starts = [base + r for r in rows_of(axis, at, line, dims)]
        if len(starts) > 1 and starts[1] - starts[0] == ne:
            return ref[starts[0] : starts[-1] + ne, :]
        return jnp.concatenate([ref[s : s + ne, :] for s in starts], 0)

    def load_plane(ref, base, axis, at, dims):
        others = [t for t in range(3) if t != axis]
        return [load_line(ref, base, axis, at, p, dims) for p in range(dims[others[0]])]

    def store_plane(ref, base, axis, at, dims, blocks):
        for p, block in enumerate(blocks):
            starts = [base + r for r in rows_of(axis, at, p, dims)]
            if starts[1] - starts[0] == ne:
                ref[starts[0] : starts[-1] + ne, :] = block
            else:
                for t, s in enumerate(starts):
                    ref[s : s + ne, :] = block[t * ne : (t + 1) * ne]

    full = [QUAD] * 3

    def mid_dims(comp):
        return [ORDER if axis == comp else QUAD for axis in range(3)]

    for comp in range(3):
        dims = dims_of(comp)
        base = comp * 48 * ne
        for a in range(ORDER):
            plane = load_plane(elem, base, comp, a, dims)
            signs = load_plane(sign, base, comp, a, dims)
            plane = [p * s for p, s in zip(plane, signs)]
            plane = apply(CLOSED, plane)
            plane = apply(CLOSED, swap(plane, ne))
            store_plane(tmp, base, comp, a, mid_dims(comp), swap(plane, ne))
        others = [t for t in range(3) if t != comp]
        for line in range(QUAD):
            xs = [load_line(tmp, base, comp, a, line, mid_dims(comp)) for a in range(ORDER)]
            for q, y in enumerate(apply(OPENED, xs)):
                starts = [comp * 64 * ne + r for r in rows_of(comp, q, line, full)]
                if starts[1] - starts[0] == ne:
                    uq[starts[0] : starts[-1] + ne, :] = y
                else:
                    for t, s in enumerate(starts):
                        uq[s : s + ne, :] = y[t * ne : (t + 1) * ne]

    part = 64 * ne

    for c in range(3):
        p, r = [t for t in range(3) if t != c]
        flipped = -1 if c == 1 else 1
        for at in range(QUAD):
            u_p = load_plane(uq, p * part, c, at, full)
            u_r = load_plane(uq, r * part, c, at, full)
            along_p = apply(COLLOC, u_r, -1)
            along_r = swap(apply(COLLOC, swap(u_p, ne), -1), ne)
            if flipped > 0:
                curl = [f - g for f, g in zip(along_p, along_r)]
            else:
                curl = [g - f for f, g in zip(along_p, along_r)]
            scale = load_plane(curlw, 0, c, at, full)
            store_plane(cq, c * part, c, at, full, [k * w for k, w in zip(curl, scale)])

    closed_t, opened_t, colloc_t = CLOSED.T, OPENED.T, COLLOC.T
    results = (res_x, res_y, res_z)
    packs = (pack2_x, pack2_y)
    rims = ((None, rim_xy, rim_xz), (rim_yx, None, rim_yz), (rim_zx, rim_zy, None))
    for res in results:
        res[...] = jnp.zeros_like(res)
    two = []
    for comp in range(3):
        dims = dims_of(comp)
        base = comp * 48 * ne
        p, r = [t for t in range(3) if t != comp]
        for at in range(QUAD):
            u = load_plane(uq, comp * part, comp, at, full)
            m = load_plane(mass, 0, comp, at, full)
            total = [a * b for a, b in zip(u, m)]
            by_p = apply(colloc_t, load_plane(cq, r * part, comp, at, full), -1)
            by_r = apply(colloc_t, swap(load_plane(cq, p * part, comp, at, full), ne), -1)
            by_r = swap(by_r, ne)
            if comp == 1:
                total = [t + a - b for t, a, b in zip(total, by_p, by_r)]
            else:
                total = [t - a + b for t, a, b in zip(total, by_p, by_r)]
            total = apply(closed_t, total)
            total = apply(closed_t, swap(total, ne))
            kept = [QUAD if axis == comp else ORDER + 1 for axis in range(3)]
            store_plane(tmp, 0, comp, at, kept, swap(total, ne))
        for line in range(ORDER + 1):
            xs = [load_line(tmp, 0, comp, q, line, kept) for q in range(QUAD)]
            for a, y in enumerate(apply(opened_t, xs)):
                y = y * load_line(sign, base, comp, a, line, dims)
                for t, s in enumerate(rows_of(comp, a, line, dims)):
                    elem[base + s : base + s + ne, :] = y[t * ne : (t + 1) * ne]
        res = results[comp]
        for x in range(res.shape[0]):
            for y in range(res.shape[1]):
                for offset, length, row, stride in places(comp, 2, (x, y, 0), 0, res.shape[2]):
                    res[x, y, offset : offset + length, :] += elem[
                        pl.ds(row, length, stride=stride), :
                    ]
        if comp < 2:
            for side in (0, 1):
                z = side * size[2]
                for x in range(res.shape[0]):
                    for y in range(res.shape[1]):
                        packs[comp][side, x, y : y + 1, :] = res[x, y, z : z + 1, :]
        for axis in range(3):
            if axis == comp:
                continue
            for side in (0, 1):
                shift = [0, 0, 0]
                shift[axis] = 2 * side - 1
                if axis == 0:
                    src = res.at[side * size[0]]
                elif axis == 1:
                    src = res.at[:, side * size[1]]
                else:
                    src = packs[comp].at[side]
                dst = rims[comp][axis].at[side]
                two.append(send(src, dst, shift, s2, r2, len(two)))
        for sp in (0, 1):
            for sr in (0, 1):
                shift = [0, 0, 0]
                shift[p], shift[r] = 2 * sp - 1, 2 * sr - 1
                where = 4 * comp + 2 * sp + sr
                if comp == 0:
                    for x in range(size[0]):
                        corner2[where, x : x + 1, :] = res[
                            x, sp * size[1], sr * size[2] : sr * size[2] + 1, :
                        ]
                    src = corner2.at[where]
                elif comp == 1:
                    for y in range(size[1]):
                        corner2[where, y : y + 1, :] = res[
                            sp * size[0], y, sr * size[2] : sr * size[2] + 1, :
                        ]
                    src = corner2.at[where]
                else:
                    src = res.at[sp * size[0], sr * size[1]]
                two.append(send(src, rc.at[where], shift, s2, r2, len(two)))

    outs = (out_x, out_y, out_z)
    for comp in range(3):
        outs[comp][...] = results[comp][...]
    for copy in two:
        copy.wait_recv()
    for comp in range(3):
        out = outs[comp]
        p, r = [t for t in range(3) if t != comp]
        for side in (0, 1):
            far = 1 - side
            if comp != 0:
                out[far * size[0]] += rims[comp][0][side]
            if comp != 1:
                for x in range(out.shape[0]):
                    out[x, far * size[1]] += rims[comp][1][side, x]
            if comp != 2:
                z = far * size[2]
                for x in range(out.shape[0]):
                    for y in range(out.shape[1]):
                        out[x, y, z : z + 1, :] += rims[comp][2][side, x, y : y + 1, :]
        for sp in (0, 1):
            for sr in (0, 1):
                where = 4 * comp + 2 * sp + sr
                fp, fr = (1 - sp) * size[p], (1 - sr) * size[r]
                if comp == 0:
                    for x in range(size[0]):
                        out[x, fp, fr : fr + 1, :] += rc[where, x : x + 1, :]
                elif comp == 1:
                    for y in range(size[1]):
                        out[fp, y, fr : fr + 1, :] += rc[where, y : y + 1, :]
                else:
                    out[fp, fr] += rc[where]
    for copy in one + two:
        copy.wait_send()


def on_device(mesh_sizes, vectors, orient_flip, reluctivity, conductivity):
    counts = (
        orient_flip.shape[0], orient_flip.shape[1], orient_flip.shape[2] // ELEM_DOFS,
    )
    ne = counts[0] * counts[1] * counts[2]
    sx, sy, sz = (ORDER * c for c in counts)
    lanes = vectors.shape[-1]
    f32 = jnp.float32
    shapes = (
        (sx, sy + 1, sz + 1, lanes), (sx + 1, sy, sz + 1, lanes), (sx + 1, sy + 1, sz, lanes),
    )
    longest = max(sx, sy, sz)
    scratch = [
        (ELEM_DOFS * ne, lanes), (ELEM_DOFS * ne, lanes), (QPTS * ne, lanes), (QPTS * ne, lanes),
        (3, ne, ELEM_DOFS), (ELEM_DOFS * ne, lanes), (3 * QPTS * ne, lanes), (3 * QPTS * ne, lanes),
        *shapes,
        (2, sx, sy, lanes), (2, longest, lanes),
        (2, sy, sz, lanes), (2, sx, sz, lanes), (2, sx, sy, lanes), (3, longest, lanes),
        (2, sx, sy + 1, lanes), (2, sx + 1, sy, lanes), (12, longest, lanes),
        (2, sx, sz + 1, lanes), (2, sx, sy + 1, lanes),
        (2, sy, sz + 1, lanes), (2, sx + 1, sy, lanes),
        (2, sy + 1, sz, lanes), (2, sx + 1, sz, lanes),
        (12, longest, lanes),
    ]
    vmem = pl.BlockSpec(memory_space=pltpu.VMEM)
    return tuple(
        pl.pallas_call(
            functools.partial(kernel, mesh_sizes),
            out_shape=[jax.ShapeDtypeStruct(s, f32) for s in shapes],
            in_specs=[vmem] * 4,
            out_specs=[vmem] * 3,
            scratch_shapes=[pltpu.VMEM(s, f32) for s in scratch]
            + [pltpu.SemaphoreType.DMA((7,))] * 2
            + [pltpu.SemaphoreType.DMA((24,))] * 2,
            compiler_params=pltpu.CompilerParams(
                collective_id=0, has_side_effects=True, vmem_limit_bytes=48 * 2**20
            ),
            name="curl_mass",
        )(vectors, orient_flip, reluctivity, conductivity)
    )


def solution(mesh):
    return jax.shard_map(
        functools.partial(on_device, tuple(mesh.shape[a] for a in AXES)),
        mesh=mesh,
        in_specs=(
            P(None, "gx", "gy", "gz", None),
            P("gx", "gy", "gz"),
            P("gx", "gy", "gz"),
            P("gx", "gy", "gz"),
        ),
        out_specs=(P("gx", "gy", "gz", None), P("gx", "gy", "gz", None), P("gx", "gy", "gz", None)),
        check_vma=False,
    )
```

```python
import functools
import jax
import jax.numpy as jnp
import numpy as np
from jax import lax
from jax.experimental import pallas as pl
from jax.experimental.pallas import tpu as pltpu
from jax.sharding import PartitionSpec as P

ORDER = 3
QUAD = 4
ELEM_DOFS = 144
QPTS = 64
AXES = ("gx", "gy", "gz")
MESH = pl.DeviceIdType.MESH
VMEM_ALL = 67043328


def lagrange(points_at, evaluate_at):
    amount = len(points_at)
    values = np.ones((len(evaluate_at), amount))
    slopes = np.zeros((len(evaluate_at), amount))
    for which in range(amount):
        for column in range(amount):
            if column != which:
                factor = (evaluate_at - points_at[column]) / (points_at[which] - points_at[column])
                slopes[:, which] = slopes[:, which] * factor + values[:, which] / (
                    points_at[which] - points_at[column]
                )
                values[:, which] = values[:, which] * factor
    return (values, slopes)


def basis_tables():
    lobatto = np.array([0.0, (1 - 5 ** (-0.5)) / 2, (1 + 5 ** (-0.5)) / 2, 1.0])
    gauss_open = np.array([(1 - 0.6**0.5) / 2, 0.5, (1 + 0.6**0.5) / 2])
    inner_pt = (3.0 / 7 - 2.0 / 7 * (6.0 / 5) ** 0.5) ** 0.5
    outer_pt = (3.0 / 7 + 2.0 / 7 * (6.0 / 5) ** 0.5) ** 0.5
    inner_wt = (18 + 30**0.5) / 36
    outer_wt = (18 - 30**0.5) / 36
    quad_points = (1 + np.array([-outer_pt, -inner_pt, inner_pt, outer_pt])) / 2
    quad_weight = np.array([outer_wt, inner_wt, inner_wt, outer_wt]) / 2
    closed, _ = lagrange(lobatto, quad_points)
    opened, _ = lagrange(gauss_open, quad_points)
    _, colloc = lagrange(quad_points, quad_points)
    return closed, opened, colloc, quad_weight


CLOSED, OPENED, COLLOC, WEIGHT = basis_tables()


def add_all(terms):
    total = terms[0]
    for term in terms[1:]:
        total = total + term
    return total


def apply(mat, xs, sigma=1):
    rows, cols = mat.shape
    half = cols // 2
    plus = [xs[p] + xs[cols - 1 - p] for p in range(half)]
    minus = [xs[p] - xs[cols - 1 - p] for p in range(half)]
    ys = [None] * rows
    for q in range((rows + 1) // 2):
        even_c = [(mat[q, p] + mat[q, cols - 1 - p]) / 2 for p in range(half)]
        odd_c = [(mat[q, p] - mat[q, cols - 1 - p]) / 2 for p in range(half)]
        even = [np.float32(c) * s for c, s in zip(even_c, plus)]
        if cols % 2:
            even.append(np.float32(mat[q, half]) * xs[half])
        even = add_all(even)
        if 2 * q == rows - 1:
            ys[q] = even
            continue
        odd = add_all([np.float32(c) * d for c, d in zip(odd_c, minus)])
        ys[q] = even + odd
        ys[rows - 1 - q] = even - odd if sigma > 0 else odd - even
    return ys


def swap(blocks, size):
    count = blocks[0].shape[0] // size
    return [
        jnp.concatenate([b[q * size : (q + 1) * size] for b in blocks], 0) for q in range(count)
    ]


def dims_of(comp):
    return [ORDER if axis == comp else ORDER + 1 for axis in range(3)]


def kernel(
    mesh_sizes, vec_hbm, flip_hbm, reluct_hbm, conduct_hbm, out_x, out_y, out_z,
    vec, flip, reluct, conduct, elem, sign, mass, curlw, flat, tmp, uq, cq,
    res_x, res_y, res_z, pack1, corner1, hx, hy, hz, hc, pack2_x, pack2_y, pack2_z, corner2,
    near_x, near_y, near_z, last_x, last_y, last_z, rc,
    s1, r1, s2, r2, s0,
):
    f32 = jnp.float32
    cx, cy = flip.shape[0], flip.shape[1]
    cz = flip.shape[2] // ELEM_DOFS
    counts = (cx, cy, cz)
    ne = cx * cy * cz
    size = tuple(ORDER * c for c in counts)
    me = [lax.axis_index(a) for a in AXES]

    def device(shift):
        return tuple(
            lax.rem(me[a] + (shift[a] + mesh_sizes[a]), mesh_sizes[a]) for a in range(3)
        )

    offsets = []
    for dx in (-1, 0, 1):
        for dy in (-1, 0, 1):
            for dz in (-1, 0, 1):
                if 1 <= abs(dx) + abs(dy) + abs(dz) <= 2:
                    offsets.append((dx, dy, dz))
    fetches = [
        pltpu.make_async_copy(src, dst, s0.at[t])
        for t, (src, dst) in enumerate(
            ((vec_hbm, vec), (flip_hbm, flip), (reluct_hbm, reluct), (conduct_hbm, conduct))
        )
    ]
    for fetch in fetches:
        fetch.start()
    barrier = pltpu.get_barrier_semaphore()
    for shift in offsets:
        pl.semaphore_signal(barrier, inc=1, device_id=device(shift), device_id_type=MESH)

    fetches[0].wait()
    for comp in (0, 1):
        for x in range(size[0]):
            for y in range(size[1]):
                pack1[comp, x, y : y + 1, :] = vec[comp, x, y, 0:1, :]
    for x in range(size[0]):
        corner1[0, x : x + 1, :] = vec[0, x, 0, 0:1, :]
    for y in range(size[1]):
        corner1[1, y : y + 1, :] = vec[1, 0, y, 0:1, :]
    pl.semaphore_wait(barrier, len(offsets))

    def send(src, dst, shift, sends, recvs, which):
        copy = pltpu.make_async_remote_copy(
            src_ref=src, dst_ref=dst, send_sem=sends.at[which], recv_sem=recvs.at[which],
            device_id=device(shift), device_id_type=MESH,
        )
        copy.start()
        return copy

    one = [
        send(corner1.at[0], hc.at[0], (0, -1, -1), s1, r1, 4),
        send(vec.at[2, 0, 0], hc.at[2], (-1, -1, 0), s1, r1, 6),
        send(corner1.at[1], hc.at[1], (-1, 0, -1), s1, r1, 5),
        send(vec.at[0, :, 0], hy.at[0], (0, -1, 0), s1, r1, 0),
        send(vec.at[2, :, 0], hy.at[1], (0, -1, 0), s1, r1, 1),
        send(pack1, hz, (0, 0, -1), s1, r1, 3),
        send(vec.at[1:3, 0], hx, (-1, 0, 0), s1, r1, 2),
    ]

    for fetch in fetches[1:]:
        fetch.wait()
    for i in range(cx):
        for j in range(cy):
            for k in range(cz):
                e = (i * cy + j) * cz + k
                flat[0, e : e + 1, 0:ELEM_DOFS] = 1.0 - 2.0 * flip[
                    i, j : j + 1, k * ELEM_DOFS : (k + 1) * ELEM_DOFS
                ].astype(f32)
                flat[1, e : e + 1, 0:QPTS] = reluct[i, j : j + 1, k * QPTS : (k + 1) * QPTS]
                flat[2, e : e + 1, 0:QPTS] = conduct[i, j : j + 1, k * QPTS : (k + 1) * QPTS]
    lanes = vec.shape[-1]
    for d in range(ELEM_DOFS):
        sign[d * ne : (d + 1) * ne, :] = jnp.broadcast_to(flat[0, :, d : d + 1], (ne, lanes))
    for q in range(QPTS):
        w = np.float32(WEIGHT[q // 16] * WEIGHT[q // 4 % 4] * WEIGHT[q % 4])
        rows = slice(q * ne, (q + 1) * ne)
        curlw[rows, :] = jnp.broadcast_to(flat[1, :, q : q + 1] * w, (ne, lanes))
        mass[rows, :] = jnp.broadcast_to(flat[2, :, q : q + 1] * w, (ne, lanes))

    def homes(comp, axis, low, high):
        found = []
        for el in range(counts[axis]):
            first = max(low, ORDER * el)
            last = min(high, ORDER * el + dims_of(comp)[axis])
            if first < last:
                found.append((el, first - ORDER * el, first - low, last - first))
        return found

    def places(comp, axis, at, low, high):
        dims = dims_of(comp)
        steps = (dims[1] * dims[2], dims[2], 1)
        span = [(p, p + 1) for p in at]
        span[axis] = (low, high)
        for fx in homes(comp, 0, *span[0]):
            for fy in homes(comp, 1, *span[1]):
                for fz in homes(comp, 2, *span[2]):
                    found = (fx, fy, fz)
                    e = (fx[0] * cy + fy[0]) * cz + fz[0]
                    d = comp * 48 + sum(found[t][1] * steps[t] for t in range(3))
                    yield found[axis][2], found[axis][3], d * ne + e, steps[axis] * ne

    def put(comp, axis, at, low, high, load):
        for offset, length, row, stride in places(comp, axis, at, low, high):
            elem[pl.ds(row, length, stride=stride), :] = load(offset, offset + length)

    for comp in range(3):
        for x in range(size[0]):
            for y in range(size[1]):
                put(comp, 2, (x, y, 0), 0, size[2], lambda a, b: vec[comp, x, y, a:b, :])

    for copy in one:
        copy.wait_recv()
    for slot, comp in ((0, 0), (1, 2)):
        for x in range(size[0]):
            put(comp, 2, (x, size[1], 0), 0, size[2], lambda a, b: hy[slot, x, a:b, :])
    for slot, comp in ((0, 1), (1, 2)):
        for y in range(size[1]):
            put(comp, 2, (size[0], y, 0), 0, size[2], lambda a, b: hx[slot, y, a:b, :])
    for comp in (0, 1):
        for x in range(size[0]):
            put(comp, 1, (x, 0, size[2]), 0, size[1], lambda a, b: hz[comp, x, a:b, :])
    put(0, 0, (0, size[1], size[2]), 0, size[0], lambda a, b: hc[0, a:b, :])
    put(1, 1, (size[0], 0, size[2]), 0, size[1], lambda a, b: hc[1, a:b, :])
    put(2, 2, (size[0], size[1], 0), 0, size[2], lambda a, b: hc[2, a:b, :])

    def rows_of(axis, at, line, dims):
        others = [t for t in range(3) if t != axis]
        points = []
        for last in range(dims[others[1]]):
            index = [0, 0, 0]
            index[axis], index[others[0]], index[others[1]] = at, line, last
            points.append(((index[0] * dims[1] + index[1]) * dims[2] + index[2]) * ne)
        return points

    def load_line(ref, base, axis, at, line, dims):
        starts = [base + r for r in rows_of(axis, at, line, dims)]
        if len(starts) > 1 and starts[1] - starts[0] == ne:
            return ref[starts[0] : starts[-1] + ne, :]
        return jnp.concatenate([ref[s : s + ne, :] for s in starts], 0)

    def load_plane(ref, base, axis, at, dims):
        others = [t for t in range(3) if t != axis]
        return [load_line(ref, base, axis, at, p, dims) for p in range(dims[others[0]])]

    def store_plane(ref, base, axis, at, dims, blocks):
        for p, block in enumerate(blocks):
            starts = [base + r for r in rows_of(axis, at, p, dims)]
            if starts[1] - starts[0] == ne:
                ref[starts[0] : starts[-1] + ne, :] = block
            else:
                for t, s in enumerate(starts):
                    ref[s : s + ne, :] = block[t * ne : (t + 1) * ne]

    full = [QUAD] * 3

    def mid_dims(comp):
        return [ORDER if axis == comp else QUAD for axis in range(3)]

    for comp in range(3):
        dims = dims_of(comp)
        base = comp * 48 * ne
        for a in range(ORDER):
            plane = load_plane(elem, base, comp, a, dims)
            signs = load_plane(sign, base, comp, a, dims)
            plane = [p * s for p, s in zip(plane, signs)]
            plane = apply(CLOSED, plane)
            plane = apply(CLOSED, swap(plane, ne))
            store_plane(tmp, base, comp, a, mid_dims(comp), swap(plane, ne))
        others = [t for t in range(3) if t != comp]
        for line in range(QUAD):
            xs = [load_line(tmp, base, comp, a, line, mid_dims(comp)) for a in range(ORDER)]
            for q, y in enumerate(apply(OPENED, xs)):
                starts = [comp * 64 * ne + r for r in rows_of(comp, q, line, full)]
                if starts[1] - starts[0] == ne:
                    uq[starts[0] : starts[-1] + ne, :] = y
                else:
                    for t, s in enumerate(starts):
                        uq[s : s + ne, :] = y[t * ne : (t + 1) * ne]

    part = 64 * ne

    for c in range(3):
        p, r = [t for t in range(3) if t != c]
        flipped = -1 if c == 1 else 1
        for at in range(QUAD):
            u_p = load_plane(uq, p * part, c, at, full)
            u_r = load_plane(uq, r * part, c, at, full)
            along_p = apply(COLLOC, u_r, -1)
            along_r = swap(apply(COLLOC, swap(u_p, ne), -1), ne)
            if flipped > 0:
                curl = [f - g for f, g in zip(along_p, along_r)]
            else:
                curl = [g - f for f, g in zip(along_p, along_r)]
            scale = load_plane(curlw, 0, c, at, full)
            store_plane(cq, c * part, c, at, full, [k * w for k, w in zip(curl, scale)])

    closed_t, opened_t, colloc_t = CLOSED.T, OPENED.T, COLLOC.T
    results = (res_x, res_y, res_z)
    packs = (pack2_x, pack2_y, pack2_z)
    near = (near_x, near_y, near_z)
    last = (last_x, last_y, last_z)
    orders = ((0, 1, 2), (0, 1, 2), (0, 2, 1))
    sends = {}
    for res in results:
        res[...] = jnp.zeros_like(res)
    for comp in (0, 2, 1):
        dims = dims_of(comp)
        base = comp * 48 * ne
        p, r = [t for t in range(3) if t != comp]
        for at in range(QUAD):
            u = load_plane(uq, comp * part, comp, at, full)
            m = load_plane(mass, 0, comp, at, full)
            total = [a * b for a, b in zip(u, m)]
            by_p = apply(colloc_t, load_plane(cq, r * part, comp, at, full), -1)
            by_r = apply(colloc_t, swap(load_plane(cq, p * part, comp, at, full), ne), -1)
            by_r = swap(by_r, ne)
            if comp == 1:
                total = [t + a - b for t, a, b in zip(total, by_p, by_r)]
            else:
                total = [t - a + b for t, a, b in zip(total, by_p, by_r)]
            total = apply(closed_t, total)
            total = apply(closed_t, swap(total, ne))
            kept = [QUAD if axis == comp else ORDER + 1 for axis in range(3)]
            store_plane(tmp, 0, comp, at, kept, swap(total, ne))
        for line in range(ORDER + 1):
            xs = [load_line(tmp, 0, comp, q, line, kept) for q in range(QUAD)]
            for a, y in enumerate(apply(opened_t, xs)):
                y = y * load_line(sign, base, comp, a, line, dims)
                for t, s in enumerate(rows_of(comp, a, line, dims)):
                    elem[base + s : base + s + ne, :] = y[t * ne : (t + 1) * ne]
        res = results[comp]
        order = orders[comp]
        for first in range(res.shape[0]):
            for middle in range(res.shape[1]):
                at = [0, 0, 0]
                at[order[0]], at[order[1]] = first, middle
                pieces = places(comp, order[2], at, 0, res.shape[2])
                for offset, length, row, stride in pieces:
                    res[first, middle, offset : offset + length, :] += elem[
                        pl.ds(row, length, stride=stride), :
                    ]
        rim = order[1] if comp == 0 else order[0]
        open_size, rim_size, last_size = size[comp], size[rim], size[order[2]]
        copies = []
        for s_rim in (0, 1):
            for s_last in (0, 1):
                shift = [0, 0, 0]
                shift[rim], shift[order[2]] = 2 * s_rim - 1, 2 * s_last - 1
                slot = 2 * s_rim + s_last
                where = 4 * comp + slot
                edge, row = s_rim * rim_size, s_last * last_size
                for t in range(open_size):
                    f, m = (t, edge) if comp == 0 else (edge, t)
                    corner2[where, t : t + 1, :] = res[f, m, row : row + 1, :]
                copies.append(
                    send(corner2.at[where], rc.at[where], shift, s2, r2, 8 * comp + slot)
                )
        for side in (0, 1):
            shift = [0, 0, 0]
            shift[rim] = 2 * side - 1
            edge = side * rim_size
            src = res.at[:, edge] if comp == 0 else res.at[edge]
            copies.append(send(src, near[comp].at[side], shift, s2, r2, 8 * comp + 4 + side))
        for side in (0, 1):
            shift = [0, 0, 0]
            shift[order[2]] = 2 * side - 1
            row = side * last_size
            for f in range(res.shape[0]):
                for m in range(res.shape[1]):
                    packs[comp][side, f, m : m + 1, :] = res[f, m, row : row + 1, :]
            copies.append(
                send(packs[comp].at[side], last[comp].at[side], shift, s2, r2, 8 * comp + 6 + side)
            )
        sends[comp] = copies

    outs = (out_x, out_y, out_z)
    for comp in range(3):
        outs[comp][...] = results[comp][...]
    for comp in (1, 0, 2):
        out, order = outs[comp], orders[comp]
        rim = order[1] if comp == 0 else order[0]
        for copy in sends[comp]:
            copy.wait_recv()
        for side in (0, 1):
            edge = (1 - side) * size[rim]
            row = (1 - side) * size[order[2]]
            if comp == 0:
                for f in range(out.shape[0]):
                    out[f, edge] += near[comp][side, f]
            else:
                out[edge] += near[comp][side]
            for f in range(out.shape[0]):
                for m in range(out.shape[1]):
                    out[f, m, row : row + 1, :] += last[comp][side, f, m : m + 1, :]
            for s_last in (0, 1):
                where = 4 * comp + 2 * side + s_last
                row = (1 - s_last) * size[order[2]]
                for t in range(size[comp]):
                    f, m = (t, edge) if comp == 0 else (edge, t)
                    out[f, m, row : row + 1, :] += rc[where, t : t + 1, :]
    for copy in one + sends[0] + sends[1] + sends[2]:
        copy.wait_send()


def write_out(from_x, from_y, from_z, to_x, to_y, to_z, sems):
    pairs = ((from_x, to_x), (from_y, to_y), (from_z, to_z))
    copies = [pltpu.make_async_copy(src, dst, sems.at[t]) for t, (src, dst) in enumerate(pairs)]
    for copy in copies:
        copy.start()
    for copy in copies:
        copy.wait()


def on_device(mesh_sizes, vectors, orient_flip, reluctivity, conductivity):
    counts = (
        orient_flip.shape[0], orient_flip.shape[1], orient_flip.shape[2] // ELEM_DOFS,
    )
    ne = counts[0] * counts[1] * counts[2]
    sx, sy, sz = (ORDER * c for c in counts)
    lanes = vectors.shape[-1]
    f32 = jnp.float32
    shapes = (
        (sx, sy + 1, sz + 1, lanes), (sx + 1, sy, sz + 1, lanes), (sx + 1, sz, sy + 1, lanes),
    )
    longest = max(sx, sy, sz)
    faces = tuple((2,) + s[:2] + (lanes,) for s in shapes)
    scratch = [
        (ELEM_DOFS * ne, lanes), (ELEM_DOFS * ne, lanes), (QPTS * ne, lanes), (QPTS * ne, lanes),
        (3, ne, ELEM_DOFS), (ELEM_DOFS * ne, lanes), (3 * QPTS * ne, lanes), (3 * QPTS * ne, lanes),
        *shapes,
        (2, sx, sy, lanes), (2, longest, lanes),
        (2, sy, sz, lanes), (2, sx, sz, lanes), (2, sx, sy, lanes), (3, longest, lanes),
        *faces, (12, longest, lanes),
        (2, sx, sz + 1, lanes), (2, sy, sz + 1, lanes), (2, sz, sy + 1, lanes),
        *faces, (12, longest, lanes),
    ]
    vmem = pl.BlockSpec(memory_space=pltpu.VMEM)
    padded = [s[0] * s[1] * (s[2] + -s[2] % 8) * lanes * 4 for s in shapes]
    room = sum(padded) + max(padded)
    anywhere = pl.BlockSpec(memory_space=pltpu.HBM)
    arguments = (vectors, orient_flip, reluctivity, conductivity)
    outs = [jax.ShapeDtypeStruct(s, f32) for s in shapes]
    held = pl.pallas_call(
        functools.partial(kernel, mesh_sizes),
        out_shape=[pltpu.VMEM(s, f32) for s in shapes],
        in_specs=[anywhere] * 4,
        out_specs=[vmem] * 3,
        scratch_shapes=[pltpu.VMEM(a.shape, a.dtype) for a in arguments]
        + [pltpu.VMEM(s, f32) for s in scratch]
        + [pltpu.SemaphoreType.DMA((7,))] * 2
        + [pltpu.SemaphoreType.DMA((24,))] * 2
        + [pltpu.SemaphoreType.DMA((4,))],
        compiler_params=pltpu.CompilerParams(
            collective_id=0, has_side_effects=True, vmem_limit_bytes=VMEM_ALL - room
        ),
        name="curl_mass",
    )(*arguments)
    held = pl.pallas_call(
        write_out,
        out_shape=outs,
        in_specs=[pl.BlockSpec(memory_space=pl.ANY)] * 3,
        out_specs=[anywhere] * 3,
        scratch_shapes=[pltpu.SemaphoreType.DMA((3,))],
        compiler_params=pltpu.CompilerParams(vmem_limit_bytes=2**20),
        name="write_out",
    )(*held)
    return held[0], held[1], jnp.swapaxes(held[2], 1, 2)


def solution(mesh):
    return jax.shard_map(
        functools.partial(on_device, tuple(mesh.shape[a] for a in AXES)),
        mesh=mesh,
        in_specs=(
            P(None, "gx", "gy", "gz", None),
            P("gx", "gy", "gz"),
            P("gx", "gy", "gz"),
            P("gx", "gy", "gz"),
        ),
        out_specs=(P("gx", "gy", "gz", None), P("gx", "gy", "gz", None), P("gx", "gy", "gz", None)),
        check_vma=False,
    )
```

```python
import functools
import jax
import jax.numpy as jnp
import numpy as np
from jax import lax
from jax.experimental import pallas as pl
from jax.experimental.pallas import tpu as pltpu
from jax.sharding import PartitionSpec as P

ORDER = 3
QUAD = 4
ELEM_DOFS = 144
QPTS = 64
AXES = ("gx", "gy", "gz")
MESH = pl.DeviceIdType.MESH
VMEM_ALL = 67043328


def lagrange(points_at, evaluate_at):
    amount = len(points_at)
    values = np.ones((len(evaluate_at), amount))
    slopes = np.zeros((len(evaluate_at), amount))
    for which in range(amount):
        for column in range(amount):
            if column != which:
                factor = (evaluate_at - points_at[column]) / (points_at[which] - points_at[column])
                slopes[:, which] = slopes[:, which] * factor + values[:, which] / (
                    points_at[which] - points_at[column]
                )
                values[:, which] = values[:, which] * factor
    return (values, slopes)


def basis_tables():
    lobatto = np.array([0.0, (1 - 5 ** (-0.5)) / 2, (1 + 5 ** (-0.5)) / 2, 1.0])
    gauss_open = np.array([(1 - 0.6**0.5) / 2, 0.5, (1 + 0.6**0.5) / 2])
    inner_pt = (3.0 / 7 - 2.0 / 7 * (6.0 / 5) ** 0.5) ** 0.5
    outer_pt = (3.0 / 7 + 2.0 / 7 * (6.0 / 5) ** 0.5) ** 0.5
    inner_wt = (18 + 30**0.5) / 36
    outer_wt = (18 - 30**0.5) / 36
    quad_points = (1 + np.array([-outer_pt, -inner_pt, inner_pt, outer_pt])) / 2
    quad_weight = np.array([outer_wt, inner_wt, inner_wt, outer_wt]) / 2
    closed, _ = lagrange(lobatto, quad_points)
    opened, _ = lagrange(gauss_open, quad_points)
    _, colloc = lagrange(quad_points, quad_points)
    return closed, opened, colloc, quad_weight


CLOSED, OPENED, COLLOC, WEIGHT = basis_tables()


def add_all(terms):
    total = terms[0]
    for term in terms[1:]:
        total = total + term
    return total


def apply(mat, xs, sigma=1):
    rows, cols = mat.shape
    half = cols // 2
    plus = [xs[p] + xs[cols - 1 - p] for p in range(half)]
    minus = [xs[p] - xs[cols - 1 - p] for p in range(half)]
    ys = [None] * rows
    for q in range((rows + 1) // 2):
        even_c = [(mat[q, p] + mat[q, cols - 1 - p]) / 2 for p in range(half)]
        odd_c = [(mat[q, p] - mat[q, cols - 1 - p]) / 2 for p in range(half)]
        even = [np.float32(c) * s for c, s in zip(even_c, plus)]
        if cols % 2:
            even.append(np.float32(mat[q, half]) * xs[half])
        even = add_all(even)
        if 2 * q == rows - 1:
            ys[q] = even
            continue
        odd = add_all([np.float32(c) * d for c, d in zip(odd_c, minus)])
        ys[q] = even + odd
        ys[rows - 1 - q] = even - odd if sigma > 0 else odd - even
    return ys


def swap(blocks, size):
    count = blocks[0].shape[0] // size
    return [
        jnp.concatenate([b[q * size : (q + 1) * size] for b in blocks], 0) for q in range(count)
    ]


def dims_of(comp):
    return [ORDER if axis == comp else ORDER + 1 for axis in range(3)]


def kernel(
    mesh_sizes, vec_hbm, flip_hbm, reluct_hbm, conduct_hbm, out_x, out_y, out_z,
    vec, flip, reluct, conduct, elem, sign, mass, curlw, flat, tmp, uq, cq,
    res_x, res_y, res_z, pack1, corner1, hx, hy, hz, hc, pack2_x, pack2_y, pack2_z, corner2,
    near_x, near_y, near_z, last_x, last_y, last_z, rc,
    s1, r1, s2, r2, s0,
):
    f32 = jnp.float32
    cx, cy = flip.shape[0], flip.shape[1]
    cz = flip.shape[2] // ELEM_DOFS
    counts = (cx, cy, cz)
    ne = cx * cy * cz
    size = tuple(ORDER * c for c in counts)
    me = [lax.axis_index(a) for a in AXES]

    def device(shift):
        return tuple(
            lax.rem(me[a] + (shift[a] + mesh_sizes[a]), mesh_sizes[a]) for a in range(3)
        )

    offsets = []
    for dx in (-1, 0, 1):
        for dy in (-1, 0, 1):
            for dz in (-1, 0, 1):
                if 1 <= abs(dx) + abs(dy) + abs(dz) <= 2:
                    offsets.append((dx, dy, dz))
    fetches = [
        pltpu.make_async_copy(src, dst, s0.at[t])
        for t, (src, dst) in enumerate(
            ((vec_hbm, vec), (flip_hbm, flip), (reluct_hbm, reluct), (conduct_hbm, conduct))
        )
    ]
    for fetch in fetches:
        fetch.start()
    barrier = pltpu.get_barrier_semaphore()
    for shift in offsets:
        pl.semaphore_signal(barrier, inc=1, device_id=device(shift), device_id_type=MESH)

    fetches[0].wait()
    for comp in (0, 1):
        for x in range(size[0]):
            for y in range(size[1]):
                pack1[comp, x, y : y + 1, :] = vec[comp, x, y, 0:1, :]
    for x in range(size[0]):
        corner1[0, x : x + 1, :] = vec[0, x, 0, 0:1, :]
    for y in range(size[1]):
        corner1[1, y : y + 1, :] = vec[1, 0, y, 0:1, :]
    pl.semaphore_wait(barrier, len(offsets))

    def send(src, dst, shift, sends, recvs, which):
        copy = pltpu.make_async_remote_copy(
            src_ref=src, dst_ref=dst, send_sem=sends.at[which], recv_sem=recvs.at[which],
            device_id=device(shift), device_id_type=MESH,
        )
        copy.start()
        return copy

    one = [
        send(corner1.at[0], hc.at[0], (0, -1, -1), s1, r1, 4),
        send(vec.at[2, 0, 0], hc.at[2], (-1, -1, 0), s1, r1, 6),
        send(corner1.at[1], hc.at[1], (-1, 0, -1), s1, r1, 5),
        send(vec.at[0, :, 0], hy.at[0], (0, -1, 0), s1, r1, 0),
        send(vec.at[2, :, 0], hy.at[1], (0, -1, 0), s1, r1, 1),
        send(pack1, hz, (0, 0, -1), s1, r1, 3),
        send(vec.at[1:3, 0], hx, (-1, 0, 0), s1, r1, 2),
    ]

    for fetch in fetches[1:]:
        fetch.wait()
    for i in range(cx):
        for j in range(cy):
            for k in range(cz):
                e = (i * cy + j) * cz + k
                flat[0, e : e + 1, 0:ELEM_DOFS] = 1.0 - 2.0 * flip[
                    i, j : j + 1, k * ELEM_DOFS : (k + 1) * ELEM_DOFS
                ].astype(f32)
                flat[1, e : e + 1, 0:QPTS] = reluct[i, j : j + 1, k * QPTS : (k + 1) * QPTS]
                flat[2, e : e + 1, 0:QPTS] = conduct[i, j : j + 1, k * QPTS : (k + 1) * QPTS]
    lanes = vec.shape[-1]
    for d in range(ELEM_DOFS):
        sign[d * ne : (d + 1) * ne, :] = jnp.broadcast_to(flat[0, :, d : d + 1], (ne, lanes))
    for q in range(QPTS):
        w = np.float32(WEIGHT[q // 16] * WEIGHT[q // 4 % 4] * WEIGHT[q % 4])
        rows = slice(q * ne, (q + 1) * ne)
        curlw[rows, :] = jnp.broadcast_to(flat[1, :, q : q + 1] * w, (ne, lanes))
        mass[rows, :] = jnp.broadcast_to(flat[2, :, q : q + 1] * w, (ne, lanes))

    def homes(comp, axis, low, high):
        found = []
        for el in range(counts[axis]):
            first = max(low, ORDER * el)
            last = min(high, ORDER * el + dims_of(comp)[axis])
            if first < last:
                found.append((el, first - ORDER * el, first - low, last - first))
        return found

    def places(comp, axis, at, low, high):
        dims = dims_of(comp)
        steps = (dims[1] * dims[2], dims[2], 1)
        span = [(p, p + 1) for p in at]
        span[axis] = (low, high)
        for fx in homes(comp, 0, *span[0]):
            for fy in homes(comp, 1, *span[1]):
                for fz in homes(comp, 2, *span[2]):
                    found = (fx, fy, fz)
                    e = (fx[0] * cy + fy[0]) * cz + fz[0]
                    d = comp * 48 + sum(found[t][1] * steps[t] for t in range(3))
                    yield found[axis][2], found[axis][3], d * ne + e, steps[axis] * ne

    def put(comp, axis, at, low, high, load):
        for offset, length, row, stride in places(comp, axis, at, low, high):
            elem[pl.ds(row, length, stride=stride), :] = load(offset, offset + length)

    for comp in range(3):
        for x in range(size[0]):
            for y in range(size[1]):
                put(comp, 2, (x, y, 0), 0, size[2], lambda a, b: vec[comp, x, y, a:b, :])

    def take_halo(comp):
        if comp == 1:
            for which in (2, 5, 6):
                one[which].wait_recv()
            for y in range(size[1]):
                put(1, 2, (size[0], y, 0), 0, size[2], lambda a, b: hx[0, y, a:b, :])
            for x in range(size[0]):
                put(1, 1, (x, 0, size[2]), 0, size[1], lambda a, b: hz[1, x, a:b, :])
            put(1, 1, (size[0], 0, size[2]), 0, size[1], lambda a, b: hc[1, a:b, :])
        elif comp == 0:
            for which in (0, 3):
                one[which].wait_recv()
            for x in range(size[0]):
                put(0, 2, (x, size[1], 0), 0, size[2], lambda a, b: hy[0, x, a:b, :])
                put(0, 1, (x, 0, size[2]), 0, size[1], lambda a, b: hz[0, x, a:b, :])
            put(0, 0, (0, size[1], size[2]), 0, size[0], lambda a, b: hc[0, a:b, :])
        else:
            for which in (1, 4):
                one[which].wait_recv()
            for x in range(size[0]):
                put(2, 2, (x, size[1], 0), 0, size[2], lambda a, b: hy[1, x, a:b, :])
            for y in range(size[1]):
                put(2, 2, (size[0], y, 0), 0, size[2], lambda a, b: hx[1, y, a:b, :])
            put(2, 2, (size[0], size[1], 0), 0, size[2], lambda a, b: hc[2, a:b, :])

    def rows_of(axis, at, line, dims):
        others = [t for t in range(3) if t != axis]
        points = []
        for last in range(dims[others[1]]):
            index = [0, 0, 0]
            index[axis], index[others[0]], index[others[1]] = at, line, last
            points.append(((index[0] * dims[1] + index[1]) * dims[2] + index[2]) * ne)
        return points

    def load_line(ref, base, axis, at, line, dims):
        starts = [base + r for r in rows_of(axis, at, line, dims)]
        if len(starts) > 1 and starts[1] - starts[0] == ne:
            return ref[starts[0] : starts[-1] + ne, :]
        return jnp.concatenate([ref[s : s + ne, :] for s in starts], 0)

    def load_plane(ref, base, axis, at, dims):
        others = [t for t in range(3) if t != axis]
        return [load_line(ref, base, axis, at, p, dims) for p in range(dims[others[0]])]

    def store_plane(ref, base, axis, at, dims, blocks):
        for p, block in enumerate(blocks):
            starts = [base + r for r in rows_of(axis, at, p, dims)]
            if starts[1] - starts[0] == ne:
                ref[starts[0] : starts[-1] + ne, :] = block
            else:
                for t, s in enumerate(starts):
                    ref[s : s + ne, :] = block[t * ne : (t + 1) * ne]

    full = [QUAD] * 3

    def mid_dims(comp):
        return [ORDER if axis == comp else QUAD for axis in range(3)]

    for comp in (1, 0, 2):
        take_halo(comp)
        dims = dims_of(comp)
        base = comp * 48 * ne
        for a in range(ORDER):
            plane = load_plane(elem, base, comp, a, dims)
            signs = load_plane(sign, base, comp, a, dims)
            plane = [p * s for p, s in zip(plane, signs)]
            plane = apply(CLOSED, plane)
            plane = apply(CLOSED, swap(plane, ne))
            store_plane(tmp, base, comp, a, mid_dims(comp), swap(plane, ne))
        others = [t for t in range(3) if t != comp]
        for line in range(QUAD):
            xs = [load_line(tmp, base, comp, a, line, mid_dims(comp)) for a in range(ORDER)]
            for q, y in enumerate(apply(OPENED, xs)):
                starts = [comp * 64 * ne + r for r in rows_of(comp, q, line, full)]
                if starts[1] - starts[0] == ne:
                    uq[starts[0] : starts[-1] + ne, :] = y
                else:
                    for t, s in enumerate(starts):
                        uq[s : s + ne, :] = y[t * ne : (t + 1) * ne]

    part = 64 * ne

    for c in range(3):
        p, r = [t for t in range(3) if t != c]
        flipped = -1 if c == 1 else 1
        for at in range(QUAD):
            u_p = load_plane(uq, p * part, c, at, full)
            u_r = load_plane(uq, r * part, c, at, full)
            along_p = apply(COLLOC, u_r, -1)
            along_r = swap(apply(COLLOC, swap(u_p, ne), -1), ne)
            if flipped > 0:
                curl = [f - g for f, g in zip(along_p, along_r)]
            else:
                curl = [g - f for f, g in zip(along_p, along_r)]
            scale = load_plane(curlw, 0, c, at, full)
            store_plane(cq, c * part, c, at, full, [k * w for k, w in zip(curl, scale)])

    closed_t, opened_t, colloc_t = CLOSED.T, OPENED.T, COLLOC.T
    results = (res_x, res_y, res_z)
    packs = (pack2_x, pack2_y, pack2_z)
    near = (near_x, near_y, near_z)
    last = (last_x, last_y, last_z)
    orders = ((0, 1, 2), (0, 1, 2), (0, 2, 1))
    sends = {}
    for res in results:
        res[...] = jnp.zeros_like(res)
    for comp in (0, 2, 1):
        dims = dims_of(comp)
        base = comp * 48 * ne
        p, r = [t for t in range(3) if t != comp]
        for at in range(QUAD):
            u = load_plane(uq, comp * part, comp, at, full)
            m = load_plane(mass, 0, comp, at, full)
            total = [a * b for a, b in zip(u, m)]
            by_p = apply(colloc_t, load_plane(cq, r * part, comp, at, full), -1)
            by_r = apply(colloc_t, swap(load_plane(cq, p * part, comp, at, full), ne), -1)
            by_r = swap(by_r, ne)
            if comp == 1:
                total = [t + a - b for t, a, b in zip(total, by_p, by_r)]
            else:
                total = [t - a + b for t, a, b in zip(total, by_p, by_r)]
            total = apply(closed_t, total)
            total = apply(closed_t, swap(total, ne))
            kept = [QUAD if axis == comp else ORDER + 1 for axis in range(3)]
            store_plane(tmp, 0, comp, at, kept, swap(total, ne))
        for line in range(ORDER + 1):
            xs = [load_line(tmp, 0, comp, q, line, kept) for q in range(QUAD)]
            for a, y in enumerate(apply(opened_t, xs)):
                y = y * load_line(sign, base, comp, a, line, dims)
                for t, s in enumerate(rows_of(comp, a, line, dims)):
                    elem[base + s : base + s + ne, :] = y[t * ne : (t + 1) * ne]
        res = results[comp]
        order = orders[comp]
        for first in range(res.shape[0]):
            for middle in range(res.shape[1]):
                at = [0, 0, 0]
                at[order[0]], at[order[1]] = first, middle
                pieces = places(comp, order[2], at, 0, res.shape[2])
                for offset, length, row, stride in pieces:
                    res[first, middle, offset : offset + length, :] += elem[
                        pl.ds(row, length, stride=stride), :
                    ]
        rim = order[1] if comp == 0 else order[0]
        open_size, rim_size, last_size = size[comp], size[rim], size[order[2]]
        copies = []
        for s_rim in (0, 1):
            for s_last in (0, 1):
                shift = [0, 0, 0]
                shift[rim], shift[order[2]] = 2 * s_rim - 1, 2 * s_last - 1
                slot = 2 * s_rim + s_last
                where = 4 * comp + slot
                edge, row = s_rim * rim_size, s_last * last_size
                for t in range(open_size):
                    f, m = (t, edge) if comp == 0 else (edge, t)
                    corner2[where, t : t + 1, :] = res[f, m, row : row + 1, :]
                copies.append(
                    send(corner2.at[where], rc.at[where], shift, s2, r2, 8 * comp + slot)
                )
        for side in (0, 1):
            shift = [0, 0, 0]
            shift[rim] = 2 * side - 1
            edge = side * rim_size
            src = res.at[:, edge] if comp == 0 else res.at[edge]
            copies.append(send(src, near[comp].at[side], shift, s2, r2, 8 * comp + 4 + side))
        for side in (0, 1):
            shift = [0, 0, 0]
            shift[order[2]] = 2 * side - 1
            row = side * last_size
            for f in range(res.shape[0]):
                for m in range(res.shape[1]):
                    packs[comp][side, f, m : m + 1, :] = res[f, m, row : row + 1, :]
            copies.append(
                send(packs[comp].at[side], last[comp].at[side], shift, s2, r2, 8 * comp + 6 + side)
            )
        sends[comp] = copies

    outs = (out_x, out_y, out_z)
    for comp in range(3):
        outs[comp][...] = results[comp][...]
    for comp in (1, 0, 2):
        out, order = outs[comp], orders[comp]
        rim = order[1] if comp == 0 else order[0]
        for copy in sends[comp]:
            copy.wait_recv()
        for side in (0, 1):
            edge = (1 - side) * size[rim]
            row = (1 - side) * size[order[2]]
            if comp == 0:
                for f in range(out.shape[0]):
                    out[f, edge] += near[comp][side, f]
            else:
                out[edge] += near[comp][side]
            for f in range(out.shape[0]):
                for m in range(out.shape[1]):
                    out[f, m, row : row + 1, :] += last[comp][side, f, m : m + 1, :]
            for s_last in (0, 1):
                where = 4 * comp + 2 * side + s_last
                row = (1 - s_last) * size[order[2]]
                for t in range(size[comp]):
                    f, m = (t, edge) if comp == 0 else (edge, t)
                    out[f, m, row : row + 1, :] += rc[where, t : t + 1, :]
    for copy in one + sends[0] + sends[1] + sends[2]:
        copy.wait_send()


def write_out(from_x, from_y, from_z, to_x, to_y, to_z, sems):
    pairs = ((from_x, to_x), (from_y, to_y), (from_z, to_z))
    copies = [pltpu.make_async_copy(src, dst, sems.at[t]) for t, (src, dst) in enumerate(pairs)]
    for copy in copies:
        copy.start()
    for copy in copies:
        copy.wait()


def on_device(mesh_sizes, vectors, orient_flip, reluctivity, conductivity):
    counts = (
        orient_flip.shape[0], orient_flip.shape[1], orient_flip.shape[2] // ELEM_DOFS,
    )
    ne = counts[0] * counts[1] * counts[2]
    sx, sy, sz = (ORDER * c for c in counts)
    lanes = vectors.shape[-1]
    f32 = jnp.float32
    shapes = (
        (sx, sy + 1, sz + 1, lanes), (sx + 1, sy, sz + 1, lanes), (sx + 1, sz, sy + 1, lanes),
    )
    longest = max(sx, sy, sz)
    faces = tuple((2,) + s[:2] + (lanes,) for s in shapes)
    scratch = [
        (ELEM_DOFS * ne, lanes), (ELEM_DOFS * ne, lanes), (QPTS * ne, lanes), (QPTS * ne, lanes),
        (3, ne, ELEM_DOFS), (ELEM_DOFS * ne, lanes), (3 * QPTS * ne, lanes), (3 * QPTS * ne, lanes),
        *shapes,
        (2, sx, sy, lanes), (2, longest, lanes),
        (2, sy, sz, lanes), (2, sx, sz, lanes), (2, sx, sy, lanes), (3, longest, lanes),
        *faces, (12, longest, lanes),
        (2, sx, sz + 1, lanes), (2, sy, sz + 1, lanes), (2, sz, sy + 1, lanes),
        *faces, (12, longest, lanes),
    ]
    vmem = pl.BlockSpec(memory_space=pltpu.VMEM)
    padded = [s[0] * s[1] * (s[2] + -s[2] % 8) * lanes * 4 for s in shapes]
    room = sum(padded) + max(padded)
    anywhere = pl.BlockSpec(memory_space=pltpu.HBM)
    arguments = (vectors, orient_flip, reluctivity, conductivity)
    outs = [jax.ShapeDtypeStruct(s, f32) for s in shapes]
    held = pl.pallas_call(
        functools.partial(kernel, mesh_sizes),
        out_shape=[pltpu.VMEM(s, f32) for s in shapes],
        in_specs=[anywhere] * 4,
        out_specs=[vmem] * 3,
        scratch_shapes=[pltpu.VMEM(a.shape, a.dtype) for a in arguments]
        + [pltpu.VMEM(s, f32) for s in scratch]
        + [pltpu.SemaphoreType.DMA((7,))] * 2
        + [pltpu.SemaphoreType.DMA((24,))] * 2
        + [pltpu.SemaphoreType.DMA((4,))],
        compiler_params=pltpu.CompilerParams(
            collective_id=0, has_side_effects=True, vmem_limit_bytes=VMEM_ALL - room
        ),
        name="curl_mass",
    )(*arguments)
    held = pl.pallas_call(
        write_out,
        out_shape=outs,
        in_specs=[pl.BlockSpec(memory_space=pl.ANY)] * 3,
        out_specs=[anywhere] * 3,
        scratch_shapes=[pltpu.SemaphoreType.DMA((3,))],
        compiler_params=pltpu.CompilerParams(vmem_limit_bytes=2**20),
        name="write_out",
    )(*held)
    return held[0], held[1], jnp.swapaxes(held[2], 1, 2)


def solution(mesh):
    return jax.shard_map(
        functools.partial(on_device, tuple(mesh.shape[a] for a in AXES)),
        mesh=mesh,
        in_specs=(
            P(None, "gx", "gy", "gz", None),
            P("gx", "gy", "gz"),
            P("gx", "gy", "gz"),
            P("gx", "gy", "gz"),
        ),
        out_specs=(P("gx", "gy", "gz", None), P("gx", "gy", "gz", None), P("gx", "gy", "gz", None)),
        check_vma=False,
    )
```
